32 devices in a mesh: exp: 8 (over z, x), dat: 4 (over y, core).
Axes of the slice: x: 2, y: 2, z: 4, core: 2. Of those that a mesh axis runs over, the one named last changes fastest.
Arguments:
- tokens: bfloat16 [4096, 1024], P(('exp', 'dat')), may hold values from -6 to 6
- norm_gain: float32 [1024], replicated, may hold values from 0.25 to 1.75
- router_weight: bfloat16 [1024, 32], P(None, 'exp'), may hold values from -0.1875 to 0.1875
- inner_weight: bfloat16 [32, 1024, 4096], P('exp', None, 'dat'), may hold values from -0.1875 to 0.1875
- outer_weight: bfloat16 [32, 4096, 1024], P('exp', 'dat'), may hold values from -0.09375 to 0.09375
- slot_tokens: int32 [32, 256], P('exp', 'dat'), may hold values from 0 to 4095, as said below
- slot_ids: int32 [4096, 2], P(('exp', 'dat')), may hold values from 0 to 8191, as said below
Outputs:
- mixed: bfloat16 [4096, 1024], P(('exp', 'dat'))
The draws below stay inside these ranges and needn't reach their ends.
Inputs may be any that keep to these rules, and one draw needn't show every extreme that they name: `slot_tokens`: column c of an expert names only tokens of the devices whose dat index is c // 64; one expert names no token twice. The 256 slots of the experts of one exp index in one dat group name tokens of any one device at most 96 times, exactly 96 times for some devices, and no times for some. Every token is named by exactly 2 slots. slot_ids[t] holds the two slots e * 256 + c with slot_tokens[e, c] = t, the smaller first.
All inputs are finite; a program needn't handle non-finite values.
Results may differ from the reference program's by a relative error of at most 0.0085.
Values may be sent and summed in bfloat16 or wider, within the bound.
A program may use at most 64 MiB of HBM per device.

```python
import jax
import jax.numpy as jnp
from jax import lax

D = 1024
FF = 4096
E_DEV = 4
TOK_DEV = 128
E = 32
C_DAT = 64
CAP = 256
TOKENS = 4096
N_EXP = 8
N_DAT = 4


def build_routes(key):
    base = jax.random.fold_in(key, 7)
    groups = N_DAT
    owners = N_EXP
    tok_rows = TOK_DEV
    spread = E_DEV * C_DAT
    average = 2 * TOK_DEV // N_EXP
    ranking = jnp.arange(owners, dtype=jnp.int32)
    profile = jnp.where(ranking < owners // 8, 3 * average, jnp.where(ranking < 3 * owners // 4, average, 0)).astype(jnp.int32)
    key_shift, key_slot, key_token = jax.random.split(base, 3)
    shifts = jax.vmap(lambda subkey: jax.random.permutation(subkey, owners))(jax.random.split(key_shift, groups)).astype(jnp.int32)
    counts = profile[(ranking[None, None, :] + shifts[:, :, None]) % owners]
    after_dev = jnp.cumsum(counts, axis=1)
    start_dev = after_dev - counts
    after_own = jnp.cumsum(counts, axis=2)
    start_own = after_own - counts
    orders = jax.vmap(lambda subkey: jax.random.permutation(subkey, spread))(jax.random.split(key_slot, groups * owners)).reshape(groups, owners, spread).astype(jnp.int32)
    circuits = jax.vmap(lambda subkey: jax.random.permutation(subkey, tok_rows))(jax.random.split(key_token, groups * owners)).reshape(groups, owners, tok_rows).astype(jnp.int32)
    owner_of = jnp.sum((after_own[:, :, None, :] <= orders[:, :, :, None]).astype(jnp.int32), axis=-1)
    within = orders - jnp.take_along_axis(start_own, owner_of, axis=2)
    position = jnp.take_along_axis(start_dev, owner_of, axis=2) + within
    flat_index = (owner_of * tok_rows + position % tok_rows).reshape(groups, owners * spread)
    local_token = jnp.take_along_axis(circuits.reshape(groups, owners * tok_rows), flat_index, axis=1).reshape(groups, owners, spread)
    group_index = jnp.arange(groups, dtype=jnp.int32)[:, None, None]
    token_id = (owner_of * groups + group_index) * tok_rows + local_token
    slot_tokens = token_id.reshape(groups, owners, E_DEV, C_DAT).transpose(1, 2, 0, 3).reshape(owners * E_DEV, groups * C_DAT)
    steps_seq = jnp.arange(2 * tok_rows, dtype=jnp.int32)
    after_by_owner = after_dev.transpose(0, 2, 1)
    device_of = jnp.sum((after_by_owner[:, :, None, :] <= steps_seq[None, None, :, None]).astype(jnp.int32), axis=-1)
    within_dev = steps_seq[None, None, :] - jnp.take_along_axis(start_dev.transpose(0, 2, 1), device_of, axis=2)
    sorted_pos = jnp.take_along_axis(start_own.transpose(0, 2, 1), device_of, axis=2) + within_dev
    inverse = jnp.argsort(orders, axis=-1).astype(jnp.int32)
    flat_slot = (device_of * spread + sorted_pos).reshape(groups, owners * 2 * tok_rows)
    slot_pos = jnp.take_along_axis(inverse.reshape(groups, owners * spread), flat_slot, axis=1).reshape(groups, owners, 2 * tok_rows)
    slot_global = (device_of * E_DEV + slot_pos // C_DAT) * CAP + group_index * C_DAT + slot_pos % C_DAT
    token_place = jnp.argsort(circuits, axis=-1).astype(jnp.int32)
    earlier_id = jnp.take_along_axis(slot_global, token_place, axis=2)
    later_id = jnp.take_along_axis(slot_global, token_place + tok_rows, axis=2)
    paired = jnp.stack([jnp.minimum(earlier_id, later_id), jnp.maximum(earlier_id, later_id)], axis=-1)
    slot_ids = paired.transpose(1, 0, 2, 3).reshape(owners * groups * tok_rows, 2)
    return (slot_tokens.astype(jnp.int32), slot_ids.astype(jnp.int32))


def draw_slot_tokens(key, part):
    return build_routes(key)[0]


def draw_slot_ids(key, part):
    return build_routes(key)[1]


def shard_levels(rng, extent, cuts, smallest, high):
    factor_of, own = 1.0, jax.random.fold_in(rng, 6)
    for dim, blocks in cuts:
        draws = jnp.exp(jax.random.uniform(jax.random.fold_in(own, dim), (blocks,), jnp.float32, smallest / len(cuts), high / len(cuts)))
        factor_of = factor_of * jnp.repeat(draws, extent[dim] // blocks).reshape([-1 if axis == dim else 1 for axis in range(len(extent))])
    return factor_of


def normal_values(own_key, extent, width, bound, cuts=(), kind=jnp.bfloat16):
    values = width * jax.random.normal(own_key, extent, jnp.float32)
    if cuts:
        values = values * shard_levels(own_key, extent, cuts, -0.22, 0.18)
    return jnp.clip(values, -bound, bound).astype(kind)


def setup_inputs(seed: int = 0) -> dict:
    keys = jax.random.split(jax.random.key(seed), 8)
    tokens = normal_values(keys[0], (TOKENS, D), 1.0, 6.0, ((0, 32),))
    norm_gain = jnp.clip(1.0 + 0.15 * jax.random.normal(keys[1], (D,), jnp.float32), 0.25, 1.75)
    router_weight = normal_values(keys[2], (D, E), D ** -0.5, 0.1875, ((1, 8),))
    inner_weight = normal_values(keys[3], (E, D, FF), D ** -0.5, 0.1875, ((0, 8), (2, 4)))
    outer_weight = normal_values(keys[4], (E, FF, D), FF ** -0.5, 0.09375, ((0, 8), (1, 4)))
    slot_tokens = draw_slot_tokens(jax.random.fold_in(keys[7], 71), 0)
    slot_ids = draw_slot_ids(jax.random.fold_in(keys[7], 71), 0)
    return dict(tokens=tokens, norm_gain=norm_gain, router_weight=router_weight, inner_weight=inner_weight, outer_weight=outer_weight, slot_tokens=slot_tokens, slot_ids=slot_ids)


EPSILON = 1e-06

def reference(tokens, norm_gain, router_weight, inner_weight, outer_weight, slot_tokens, slot_ids):
    values = tokens.astype(jnp.float32)
    scale = lax.rsqrt(lax.optimization_barrier(jnp.mean(values * values, axis=-1, keepdims=True)) + EPSILON)
    normed = (values * scale * norm_gain.astype(jnp.float32)).astype(jnp.bfloat16)
    slot_rows = jnp.take(normed, slot_tokens, axis=0)
    gate_score = jax.nn.sigmoid(jnp.einsum('ecd,de->ec', slot_rows.astype(jnp.float32), router_weight.astype(jnp.float32)))
    capacity = slot_tokens.shape[1]
    ff_block = FF // N_DAT

    def expert(inputs):
        block, first_weight, second_weight = inputs
        hidden = jax.nn.relu(jnp.dot(block, first_weight, preferred_element_type=jnp.float32)).astype(jnp.bfloat16)
        pieces = hidden.reshape(capacity, N_DAT, ff_block).astype(jnp.float32)
        seconds = second_weight.reshape(N_DAT, ff_block, D).astype(jnp.float32)
        partial_sums = jnp.einsum('ckf,kfd->kcd', pieces, seconds).astype(jnp.bfloat16)
        partial_sums = lax.optimization_barrier(partial_sums)
        return lax.optimization_barrier(jnp.sum(partial_sums.astype(jnp.float32), axis=0))
    expert_out = lax.map(expert, (slot_rows, inner_weight, outer_weight))
    weighted = (gate_score[:, :, None] * expert_out).astype(jnp.bfloat16).reshape(-1, D)
    chosen = jnp.take(weighted, slot_ids.reshape(-1), axis=0).reshape(slot_ids.shape[0], 2, D).astype(jnp.float32)
    combined = chosen[:, 0] + chosen[:, 1]
    return (values + combined).astype(jnp.bfloat16)
```

```python
import jax
import jax.numpy as jnp
from jax import lax
from jax.experimental import pallas as pl
from jax.experimental.pallas import tpu as pltpu
from jax.sharding import PartitionSpec as P

EPSILON = 1e-06


def normalize(tokens, norm_gain):
    values = tokens.astype(jnp.float32)
    scale = lax.rsqrt(jnp.mean(values * values, axis=-1, keepdims=True) + EPSILON)
    return (values * scale * norm_gain).astype(jnp.bfloat16)


def owner_places(slot_ids, experts_dev, capacity, bucket):
    flat_ids = slot_ids.reshape(-1)
    source = flat_ids // capacity // experts_dev
    before = (source[:, None] == source[None, :]) & (flat_ids[None, :] < flat_ids[:, None])
    ranks_in = jnp.sum(before.astype(jnp.int32), axis=1)
    return (source * bucket + ranks_in).reshape(slot_ids.shape)


def expert_places(token_ids, slot_keys, tok_rows, dat_count, bucket):
    owner_of = token_ids // (tok_rows * dat_count)
    before = (owner_of[:, None] == owner_of[None, :]) & (slot_keys[None, :] < slot_keys[:, None])
    ranks_in = jnp.sum(before.astype(jnp.int32), axis=1)
    return owner_of * bucket + ranks_in


def body(tokens, norm_gain, router_weight, inner_weight, outer_weight, slot_tokens, slot_ids):
    exp_count = lax.axis_size("exp")
    dat_count = lax.axis_size("dat")
    tok_rows, width = tokens.shape
    experts_dev, cap_dev = slot_tokens.shape
    bucket = 6 * tok_rows // exp_count
    normed = normalize(tokens, norm_gain)
    picked = slot_tokens.T.reshape(-1)
    expert_iota = lax.broadcasted_iota(jnp.int32, (cap_dev, experts_dev), 1)
    column_iota = lax.broadcasted_iota(jnp.int32, (cap_dev, experts_dev), 0)
    slot_keys = (expert_iota * cap_dev + column_iota).reshape(-1)
    senders = expert_places(picked, slot_keys, tok_rows, dat_count, bucket)
    receivers = owner_places(slot_ids, experts_dev, cap_dev * dat_count, bucket)
    lookup = jnp.any(
        lax.broadcasted_iota(jnp.int32, (exp_count * bucket, 1, 1), 0) == receivers[None], axis=2
    )
    outgoing = jnp.dot(lookup.astype(jnp.bfloat16), normed, preferred_element_type=jnp.float32)
    outgoing = outgoing.astype(jnp.bfloat16).reshape(exp_count, bucket, width)
    arrived = lax.all_to_all(outgoing, "exp", split_axis=0, concat_axis=0, tiled=True).reshape(
        exp_count * bucket, width
    )
    gathered_rows = jnp.take(arrived, senders, axis=0)
    gathered_rows = gathered_rows.reshape(cap_dev, experts_dev, width)
    gate_score = jax.nn.sigmoid(
        jnp.einsum("ced,de->ce", gathered_rows, router_weight, preferred_element_type=jnp.float32)
    )
    inner = jnp.einsum(
        "ced,edf->cef",
        lax.all_gather(gathered_rows, "dat", axis=0, tiled=True),
        inner_weight,
        preferred_element_type=jnp.float32,
    )
    hidden = jax.nn.relu(inner).astype(jnp.bfloat16)
    expert_out = lax.psum_scatter(
        jnp.einsum("cef,efd->ced", hidden, outer_weight, preferred_element_type=jnp.float32).astype(
            jnp.bfloat16
        ),
        "dat",
        scatter_dimension=0,
        tiled=True,
    ).astype(jnp.float32)
    weighted = (gate_score[:, :, None] * expert_out).astype(jnp.bfloat16).reshape(-1, width)
    placing = lax.broadcasted_iota(jnp.int32, (exp_count * bucket, 1), 0) == senders[None, :]
    returning = jnp.dot(placing.astype(jnp.bfloat16), weighted, preferred_element_type=jnp.float32)
    returning = returning.astype(jnp.bfloat16).reshape(exp_count, bucket, width)
    came_back = lax.all_to_all(returning, "exp", split_axis=0, concat_axis=0, tiled=True).reshape(
        exp_count * bucket, width
    )
    combine_table = jnp.sum(
        (
            lax.broadcasted_iota(jnp.int32, (1, 1, exp_count * bucket), 2) == receivers[:, :, None]
        ).astype(jnp.float32),
        axis=1,
    )
    combined = jnp.dot(
        combine_table.astype(jnp.bfloat16), came_back, preferred_element_type=jnp.float32
    )
    return (tokens.astype(jnp.float32) + combined).astype(jnp.bfloat16)


MESH = pl.DeviceIdType.MESH
PAIR = 2
CHUNK = 256


def moe_kernel(
    tokens_ref, gain_ref, router_ref, ids_ref, inner_hbm, outer_hbm, out_ref,
    inner_v, outer_v, ids_far, pick, place, blocks, own_part, far_send, far_recv,
    rows, hidden, gate, parts, core_recv, y_send, y_recv, kept, weighted, x_recv,
    dense, up_send, up_recv, down_send, down_recv,
    w_sem, ids_sem, zu_sem, zd_sem, x_sem, y_sem, c_sem, cr_sem,
    rc_sem, ry_sem, rx_sem, ru_sem, rd_sem,
):
    chunks, lines, tok_rows, wide = blocks.shape
    experts_dev = inner_v.shape[0]
    slots = weighted.shape[1]
    cap_dev = slots // experts_dev
    exp = lax.axis_index("exp")
    dat = lax.axis_index("dat")
    dat_count = lax.axis_size("dat")
    z, x = exp // PAIR, exp % PAIR
    y, c = dat // PAIR, dat % PAIR
    up = (exp + PAIR, dat)
    down = (exp - PAIR, dat)
    x_peer = (exp + 1 - 2 * x, dat)
    y_peer = (exp, dat + PAIR - 2 * PAIR * y)
    c_peer = (exp, dat + 1 - 2 * c)
    has_up = z + 1 < lines
    has_down = z > 0
    sent = []

    def copy_to(src, dst, sems, where, peer):
        return pltpu.make_async_remote_copy(
            src_ref=src, dst_ref=dst, send_sem=sems.at[(0,) + where],
            recv_sem=sems.at[(1,) + where], device_id=peer, device_id_type=MESH,
        )

    def send(copy, cond=None):
        sent.append((copy, cond))
        if cond is None:
            copy.start()
        else:
            pl.when(cond)(copy.start)

    loads = []
    for e in range(experts_dev):
        loads.append(pltpu.make_async_copy(inner_hbm.at[e], inner_v.at[e], w_sem.at[0, e]))
    for e in range(experts_dev):
        loads.append(pltpu.make_async_copy(outer_hbm.at[e], outer_v.at[e], w_sem.at[1, e]))
    for load in loads:
        load.start()

    barrier = pltpu.get_barrier_semaphore()
    for peer in (x_peer, y_peer, c_peer):
        pl.semaphore_signal(barrier, inc=1, device_id=peer, device_id_type=MESH)

    @pl.when(has_up)
    def _():
        pl.semaphore_signal(barrier, inc=1, device_id=up, device_id_type=MESH)

    @pl.when(has_down)
    def _():
        pl.semaphore_signal(barrier, inc=1, device_id=down, device_id_type=MESH)

    values = tokens_ref[...].astype(jnp.float32)
    scale = lax.rsqrt(jnp.mean(values * values, axis=-1, keepdims=True) + EPSILON)
    normed = (values * scale * gain_ref[...]).astype(jnp.bfloat16)
    for j in range(chunks):
        blocks[j, z] = normed[:, j * wide : (j + 1) * wide]

    pl.semaphore_wait(barrier, 3 + has_up.astype(jnp.int32) + has_down.astype(jnp.int32))

    ids_copy = copy_to(ids_ref, ids_far, ids_sem, (), x_peer)

    def one_hots(side, ids):
        for s in range(lines):
            base = ((s * PAIR + x) * dat_count + dat) * tok_rows
            local = lax.broadcasted_iota(jnp.int32, (tok_rows, slots), 0) + base
            hot = (ids[0:1, :] == local).astype(jnp.float32)
            place[side, s * tok_rows : (s + 1) * tok_rows, :] = hot.astype(jnp.bfloat16)
            pick[side, :, s * tok_rows : (s + 1) * tok_rows] = hot.T.astype(jnp.bfloat16)

    def own_rows(j, of_dat):
        return rows.at[j, :, pl.ds(pl.multiple_of(of_dat * cap_dev, cap_dev), cap_dev), :]

    dat_y = dat + PAIR - 2 * PAIR * y
    dat_c = dat + 1 - 2 * c
    dat_yc = dat_y + 1 - 2 * c

    for t in range(chunks + lines + 2):
        if t < chunks:
            send(copy_to(blocks.at[t, z], blocks.at[t, z], zu_sem, (t, z), up), has_up)
            send(copy_to(blocks.at[t, z], blocks.at[t, z], zd_sem, (t, z), down), has_down)
        if t == 0:
            send(ids_copy)
            one_hots(0, ids_ref)
        if t == 1:
            ids_copy.wait_recv()
            one_hots(1, ids_far)
        for k in range(1, lines):
            j = t - k
            if 0 <= j < chunks:
                low, high = z - k, z + k
                from_low = copy_to(blocks.at[j, low], blocks.at[j, low], zu_sem, (j, low), up)
                from_high = copy_to(blocks.at[j, high], blocks.at[j, high], zd_sem, (j, high), down)
                pl.when(low >= 0)(from_low.wait_recv)
                if k + 1 < lines:
                    send(from_low, (low >= 0) & has_up)
                pl.when(high < lines)(from_high.wait_recv)
                if k + 1 < lines:
                    send(from_high, (high < lines) & has_down)
        j = t - (lines - 1)
        if 0 <= j < chunks:
            found = blocks[j].reshape(lines * tok_rows, wide)
            far_send[j] = jnp.dot(pick[1], found, preferred_element_type=jnp.float32).astype(jnp.bfloat16)
            send(copy_to(far_send.at[j], far_recv.at[j], x_sem, (j,), x_peer))
            own_part[j] = jnp.dot(pick[0], found, preferred_element_type=jnp.float32)
        j = t - lines
        if 0 <= j < chunks:
            copy_to(far_send.at[j], far_recv.at[j], x_sem, (j,), x_peer).wait_recv()
            merged = (own_part[j] + far_recv[j].astype(jnp.float32)).astype(jnp.bfloat16)
            own_rows(j, dat)[...] = merged.reshape(experts_dev, cap_dev, wide)
            send(copy_to(own_rows(j, dat), own_rows(j, dat), y_sem, (j,), y_peer))
            send(copy_to(own_rows(j, dat), own_rows(j, dat), c_sem, (j,), c_peer))
            score = jnp.dot(
                merged, router_ref[j * wide : (j + 1) * wide, :], preferred_element_type=jnp.float32
            )
            row_id = lax.broadcasted_iota(jnp.int32, score.shape, 0)
            first = lax.broadcasted_iota(jnp.int32, score.shape, 1) * cap_dev
            mine = (row_id >= first) & (row_id < first + cap_dev)
            score = jnp.sum(jnp.where(mine, score, 0.0), axis=1, keepdims=True)
            gate[...] = score if j == 0 else gate[...] + score
        j = t - lines - 1
        if 0 <= j < chunks:
            copy_to(own_rows(j, dat_y), own_rows(j, dat_y), y_sem, (j,), y_peer).wait_recv()
            send(copy_to(own_rows(j, dat_y), own_rows(j, dat_y), cr_sem, (j,), c_peer))
    gate[...] = jax.nn.sigmoid(gate[...])
    for j in range(chunks):
        copy_to(own_rows(j, dat_c), own_rows(j, dat_c), c_sem, (j,), c_peer).wait_recv()
        copy_to(own_rows(j, dat_yc), own_rows(j, dat_yc), cr_sem, (j,), c_peer).wait_recv()
    for load in loads:
        load.wait()

    @pl.loop(0, experts_dev)
    def _(e):
        total = jnp.dot(rows[0, e], inner_v[e, :wide, :], preferred_element_type=jnp.float32)
        for j in range(1, chunks):
            total += jnp.dot(
                rows[j, e], inner_v[e, j * wide : (j + 1) * wide, :], preferred_element_type=jnp.float32
            )
        hidden[e] = jnp.maximum(total, 0.0).astype(jnp.bfloat16)

    def block(s):
        return slice(s * tok_rows, (s + 1) * tok_rows)

    for t in range(chunks + 4 + lines):
        j = t
        if j < chunks:

            @pl.loop(0, experts_dev)
            def _(e, j=j):
                part = jnp.dot(
                    hidden[e], outer_v[e, :, j * wide : (j + 1) * wide], preferred_element_type=jnp.float32
                ).astype(jnp.bfloat16)
                for d in range(PAIR * PAIR):
                    parts[j, d // PAIR, d % PAIR, e] = part[d * cap_dev : (d + 1) * cap_dev, :]

            send(copy_to(parts.at[j, :, 1 - c], core_recv.at[j], rc_sem, (j,), c_peer))
        j = t - 1
        if 0 <= j < chunks:
            copy_to(parts.at[j, :, 1 - c], core_recv.at[j], rc_sem, (j,), c_peer).wait_recv()
            theirs = parts[j, 1 - y, c].astype(jnp.float32) + core_recv[j, 1 - y].astype(jnp.float32)
            y_send[j] = theirs.astype(jnp.bfloat16).reshape(slots, wide)
            send(copy_to(y_send.at[j], y_recv.at[j], ry_sem, (j,), y_peer))
            ours = parts[j, y, c].astype(jnp.float32) + core_recv[j, y].astype(jnp.float32)
            kept[j] = ours.reshape(slots, wide)
        j = t - 2
        if 0 <= j < chunks:
            copy_to(y_send.at[j], y_recv.at[j], ry_sem, (j,), y_peer).wait_recv()
            summed = kept[j] + y_recv[j].astype(jnp.float32)
            weighted[j] = (gate[...] * summed).astype(jnp.bfloat16)
            send(copy_to(weighted.at[j], x_recv.at[j], rx_sem, (j,), x_peer))
        j = t - 3
        if 0 <= j < chunks:
            copy_to(weighted.at[j], x_recv.at[j], rx_sem, (j,), x_peer).wait_recv()
            spread = jnp.dot(place[0], weighted[j], preferred_element_type=jnp.float32)
            spread += jnp.dot(place[1], x_recv[j], preferred_element_type=jnp.float32)
            dense[j] = spread
        for s in range(lines):
            j = t - 3 - s
            if not 0 <= j < chunks:
                continue
            for dest in range(lines - 1, s, -1):
                here = z == s
                go = copy_to(up_send.at[j, dest], up_recv.at[j, dest], ru_sem, (j, dest), up)

                @pl.when(here)
                def _(j=j, dest=dest, s=s, go=go):
                    total = dense[j, block(dest), :]
                    if s > 0:
                        go.wait_recv()
                        total += up_recv[j, dest].astype(jnp.float32)
                    up_send[j, dest] = total.astype(jnp.bfloat16)

                send(go, here)
            top = lines - 1 - s
            for dest in range(top):
                here = z == top
                go = copy_to(down_send.at[j, dest], down_recv.at[j, dest], rd_sem, (j, dest), down)

                @pl.when(here)
                def _(j=j, dest=dest, top=top, go=go):
                    total = dense[j, block(dest), :]
                    if top < lines - 1:
                        go.wait_recv()
                        total += down_recv[j, dest].astype(jnp.float32)
                    down_send[j, dest] = total.astype(jnp.bfloat16)

                send(go, here)
        j = t - 3 - lines
        if 0 <= j < chunks:
            for s in range(lines):

                @pl.when(z == s)
                def _(j=j, s=s):
                    cols = slice(j * wide, (j + 1) * wide)
                    total = dense[j, block(s), :]
                    if s > 0:
                        copy_to(up_send.at[j, s], up_recv.at[j, s], ru_sem, (j, s), up).wait_recv()
                        total += up_recv[j, s].astype(jnp.float32)
                    if s < lines - 1:
                        copy_to(down_send.at[j, s], down_recv.at[j, s], rd_sem, (j, s), down).wait_recv()
                        total += down_recv[j, s].astype(jnp.float32)
                    out_ref[:, cols] = (tokens_ref[:, cols].astype(jnp.float32) + total).astype(jnp.bfloat16)

    for copy, cond in sent:
        if cond is None:
            copy.wait_send()
        else:
            pl.when(cond)(copy.wait_send)


def kernel_body(tokens, norm_gain, router_weight, inner_weight, outer_weight, slot_tokens, slot_ids):
    del slot_ids
    tok_rows, width = tokens.shape
    experts_dev, cap_dev = slot_tokens.shape
    units = inner_weight.shape[2]
    lines = lax.axis_size("exp") // PAIR
    dat_count = lax.axis_size("dat")
    slots = experts_dev * cap_dev
    chunks = width // CHUNK
    ids = jnp.broadcast_to(slot_tokens.reshape(1, slots), (8, slots))
    bf16, f32 = jnp.bfloat16, jnp.float32
    vmem = pl.BlockSpec(memory_space=pltpu.VMEM)
    hbm = pl.BlockSpec(memory_space=pl.ANY)
    dma = pltpu.SemaphoreType.DMA
    return pl.pallas_call(
        moe_kernel,
        out_shape=jax.ShapeDtypeStruct((tok_rows, width), bf16),
        in_specs=[vmem, vmem, vmem, vmem, hbm, hbm],
        out_specs=vmem,
        scratch_shapes=[
            pltpu.VMEM((experts_dev, width, units), bf16),
            pltpu.VMEM((experts_dev, units, width), bf16),
            pltpu.VMEM((8, slots), jnp.int32),
            pltpu.VMEM((2, slots, lines * tok_rows), bf16),
            pltpu.VMEM((2, lines * tok_rows, slots), bf16),
            pltpu.VMEM((chunks, lines, tok_rows, CHUNK), bf16),
            pltpu.VMEM((chunks, slots, CHUNK), f32),
            pltpu.VMEM((chunks, slots, CHUNK), bf16),
            pltpu.VMEM((chunks, slots, CHUNK), bf16),
            pltpu.VMEM((chunks, experts_dev, dat_count * cap_dev, CHUNK), bf16),
            pltpu.VMEM((experts_dev, dat_count * cap_dev, units), bf16),
            pltpu.VMEM((slots, 1), f32),
            pltpu.VMEM((chunks, PAIR, PAIR, experts_dev, cap_dev, CHUNK), bf16),
            pltpu.VMEM((chunks, PAIR, experts_dev, cap_dev, CHUNK), bf16),
            pltpu.VMEM((chunks, slots, CHUNK), bf16),
            pltpu.VMEM((chunks, slots, CHUNK), bf16),
            pltpu.VMEM((chunks, slots, CHUNK), f32),
            pltpu.VMEM((chunks, slots, CHUNK), bf16),
            pltpu.VMEM((chunks, slots, CHUNK), bf16),
            pltpu.VMEM((chunks, lines * tok_rows, CHUNK), f32),
            pltpu.VMEM((chunks, lines, tok_rows, CHUNK), bf16),
            pltpu.VMEM((chunks, lines, tok_rows, CHUNK), bf16),
            pltpu.VMEM((chunks, lines, tok_rows, CHUNK), bf16),
            pltpu.VMEM((chunks, lines, tok_rows, CHUNK), bf16),
            dma((2, experts_dev)),
            dma((2,)),
            dma((2, chunks, lines)),
            dma((2, chunks, lines)),
            dma((2, chunks)),
            dma((2, chunks)),
            dma((2, chunks)),
            dma((2, chunks)),
            dma((2, chunks)),
            dma((2, chunks)),
            dma((2, chunks)),
            dma((2, chunks, lines)),
            dma((2, chunks, lines)),
        ],
        compiler_params=pltpu.CompilerParams(
            collective_id=0, has_side_effects=True, vmem_limit_bytes=60 * 1024 * 1024
        ),
    )(tokens, norm_gain.reshape(1, width), router_weight, ids, inner_weight, outer_weight)


def solution(mesh):
    chosen = kernel_body if mesh.shape["dat"] == PAIR * PAIR else body
    in_specs = (
        P(("exp", "dat"), None),
        P(),
        P(None, "exp"),
        P("exp", None, "dat"),
        P("exp", "dat", None),
        P("exp", "dat"),
        P(("exp", "dat"), None),
    )
    out_specs = P(("exp", "dat"), None)
    return jax.shard_map(chosen, mesh=mesh, in_specs=in_specs, out_specs=out_specs, check_vma=False)
```

```python
import jax
import jax.numpy as jnp
from jax import lax
from jax.experimental import pallas as pl
from jax.experimental.pallas import tpu as pltpu
from jax.sharding import PartitionSpec as P

EPSILON = 1e-06


def normalize(tokens, norm_gain):
    values = tokens.astype(jnp.float32)
    scale = lax.rsqrt(jnp.mean(values * values, axis=-1, keepdims=True) + EPSILON)
    return (values * scale * norm_gain).astype(jnp.bfloat16)


def owner_places(slot_ids, experts_dev, capacity, bucket):
    flat_ids = slot_ids.reshape(-1)
    source = flat_ids // capacity // experts_dev
    before = (source[:, None] == source[None, :]) & (flat_ids[None, :] < flat_ids[:, None])
    ranks_in = jnp.sum(before.astype(jnp.int32), axis=1)
    return (source * bucket + ranks_in).reshape(slot_ids.shape)


def expert_places(token_ids, slot_keys, tok_rows, dat_count, bucket):
    owner_of = token_ids // (tok_rows * dat_count)
    before = (owner_of[:, None] == owner_of[None, :]) & (slot_keys[None, :] < slot_keys[:, None])
    ranks_in = jnp.sum(before.astype(jnp.int32), axis=1)
    return owner_of * bucket + ranks_in


def body(tokens, norm_gain, router_weight, inner_weight, outer_weight, slot_tokens, slot_ids):
    exp_count = lax.axis_size("exp")
    dat_count = lax.axis_size("dat")
    tok_rows, width = tokens.shape
    experts_dev, cap_dev = slot_tokens.shape
    bucket = 6 * tok_rows // exp_count
    normed = normalize(tokens, norm_gain)
    picked = slot_tokens.T.reshape(-1)
    expert_iota = lax.broadcasted_iota(jnp.int32, (cap_dev, experts_dev), 1)
    column_iota = lax.broadcasted_iota(jnp.int32, (cap_dev, experts_dev), 0)
    slot_keys = (expert_iota * cap_dev + column_iota).reshape(-1)
    senders = expert_places(picked, slot_keys, tok_rows, dat_count, bucket)
    receivers = owner_places(slot_ids, experts_dev, cap_dev * dat_count, bucket)
    lookup = jnp.any(
        lax.broadcasted_iota(jnp.int32, (exp_count * bucket, 1, 1), 0) == receivers[None], axis=2
    )
    outgoing = jnp.dot(lookup.astype(jnp.bfloat16), normed, preferred_element_type=jnp.float32)
    outgoing = outgoing.astype(jnp.bfloat16).reshape(exp_count, bucket, width)
    arrived = lax.all_to_all(outgoing, "exp", split_axis=0, concat_axis=0, tiled=True).reshape(
        exp_count * bucket, width
    )
    gathered_rows = jnp.take(arrived, senders, axis=0)
    gathered_rows = gathered_rows.reshape(cap_dev, experts_dev, width)
    gate_score = jax.nn.sigmoid(
        jnp.einsum("ced,de->ce", gathered_rows, router_weight, preferred_element_type=jnp.float32)
    )
    inner = jnp.einsum(
        "ced,edf->cef",
        lax.all_gather(gathered_rows, "dat", axis=0, tiled=True),
        inner_weight,
        preferred_element_type=jnp.float32,
    )
    hidden = jax.nn.relu(inner).astype(jnp.bfloat16)
    expert_out = lax.psum_scatter(
        jnp.einsum("cef,efd->ced", hidden, outer_weight, preferred_element_type=jnp.float32).astype(
            jnp.bfloat16
        ),
        "dat",
        scatter_dimension=0,
        tiled=True,
    ).astype(jnp.float32)
    weighted = (gate_score[:, :, None] * expert_out).astype(jnp.bfloat16).reshape(-1, width)
    placing = lax.broadcasted_iota(jnp.int32, (exp_count * bucket, 1), 0) == senders[None, :]
    returning = jnp.dot(placing.astype(jnp.bfloat16), weighted, preferred_element_type=jnp.float32)
    returning = returning.astype(jnp.bfloat16).reshape(exp_count, bucket, width)
    came_back = lax.all_to_all(returning, "exp", split_axis=0, concat_axis=0, tiled=True).reshape(
        exp_count * bucket, width
    )
    combine_table = jnp.sum(
        (
            lax.broadcasted_iota(jnp.int32, (1, 1, exp_count * bucket), 2) == receivers[:, :, None]
        ).astype(jnp.float32),
        axis=1,
    )
    combined = jnp.dot(
        combine_table.astype(jnp.bfloat16), came_back, preferred_element_type=jnp.float32
    )
    return (tokens.astype(jnp.float32) + combined).astype(jnp.bfloat16)


MESH = pl.DeviceIdType.MESH
PAIR = 2
CHUNK = 256
GROUP = 256


def moe_kernel(
    tokens_ref, gain_ref, router_ref, ids_ref, inner_hbm, outer_hbm, out_ref,
    inner_v, outer_v, ids_far, pick, place, blocks, own_part, far_send, far_recv,
    rows, sums, hidden, gate, parts, core_recv, y_send, y_recv, kept, weighted, x_recv,
    dense, up_send, up_recv, down_send, down_recv,
    w_sem, ids_sem, zu_sem, zd_sem, x_sem, y_sem, c_sem, cr_sem,
    rc_sem, ry_sem, rx_sem, ru_sem, rd_sem,
):
    chunks, lines, tok_rows, wide = blocks.shape
    experts_dev = inner_v.shape[0]
    slots = weighted.shape[1]
    groups, span = rows.shape[0], rows.shape[3]
    per = span // wide
    cap_dev = slots // experts_dev
    exp = lax.axis_index("exp")
    dat = lax.axis_index("dat")
    dat_count = lax.axis_size("dat")
    z, x = exp // PAIR, exp % PAIR
    y, c = dat // PAIR, dat % PAIR
    up = (exp + PAIR, dat)
    down = (exp - PAIR, dat)
    x_peer = (exp + 1 - 2 * x, dat)
    y_peer = (exp, dat + PAIR - 2 * PAIR * y)
    c_peer = (exp, dat + 1 - 2 * c)
    has_up = z + 1 < lines
    has_down = z > 0
    sent = []

    def copy_to(src, dst, sems, where, peer):
        return pltpu.make_async_remote_copy(
            src_ref=src, dst_ref=dst, send_sem=sems.at[(0,) + where],
            recv_sem=sems.at[(1,) + where], device_id=peer, device_id_type=MESH,
        )

    def send(copy, cond=None):
        sent.append((copy, cond))
        if cond is None:
            copy.start()
        else:
            pl.when(cond)(copy.start)

    loads = []
    for e in range(experts_dev):
        loads.append(pltpu.make_async_copy(inner_hbm.at[e], inner_v.at[e], w_sem.at[0, e]))
    for e in range(experts_dev):
        loads.append(pltpu.make_async_copy(outer_hbm.at[e], outer_v.at[e], w_sem.at[1, e]))
    for load in loads:
        load.start()

    barrier = pltpu.get_barrier_semaphore()
    for peer in (x_peer, y_peer, c_peer):
        pl.semaphore_signal(barrier, inc=1, device_id=peer, device_id_type=MESH)

    @pl.when(has_up)
    def _():
        pl.semaphore_signal(barrier, inc=1, device_id=up, device_id_type=MESH)

    @pl.when(has_down)
    def _():
        pl.semaphore_signal(barrier, inc=1, device_id=down, device_id_type=MESH)

    values = tokens_ref[...].astype(jnp.float32)
    scale = lax.rsqrt(jnp.mean(values * values, axis=-1, keepdims=True) + EPSILON)
    normed = (values * scale * gain_ref[...]).astype(jnp.bfloat16)
    for j in range(chunks):
        blocks[j, z] = normed[:, j * wide : (j + 1) * wide]

    pl.semaphore_wait(barrier, 3 + has_up.astype(jnp.int32) + has_down.astype(jnp.int32))

    ids_copy = copy_to(ids_ref, ids_far, ids_sem, (), x_peer)

    def one_hots(side, ids):
        for s in range(lines):
            base = ((s * PAIR + x) * dat_count + dat) * tok_rows
            local = lax.broadcasted_iota(jnp.int32, (tok_rows, slots), 0) + base
            all_ids = jnp.concatenate([ids[e : e + 1, :] for e in range(experts_dev)], axis=1)
            hot = (all_ids == local).astype(jnp.float32)
            place[side, s * tok_rows : (s + 1) * tok_rows, :] = hot.astype(jnp.bfloat16)
            pick[side, :, s * tok_rows : (s + 1) * tok_rows] = hot.T.astype(jnp.bfloat16)

    def own_rows(j, of_dat):
        first = (j % per) * wide
        at = pl.ds(pl.multiple_of(of_dat * cap_dev, cap_dev), cap_dev)
        return rows.at[j // per, :, at, first : first + wide]

    def first_product(g):
        if g == 0:
            for e in range(experts_dev):
                loads[e].wait()

        @pl.loop(0, experts_dev, unroll=True)
        def _(e):
            total = jnp.dot(
                rows[g, e], inner_v[e, g * span : (g + 1) * span, :], preferred_element_type=jnp.float32
            )
            if g > 0:
                total += sums[e]
            if g + 1 < groups:
                sums[e] = total
            else:
                hidden[e] = jnp.maximum(total, 0.0).astype(jnp.bfloat16)

    dat_y = dat + PAIR - 2 * PAIR * y
    dat_c = dat + 1 - 2 * c
    dat_yc = dat_y + 1 - 2 * c

    for t in range(chunks + lines + 3):
        if t < chunks:
            send(copy_to(blocks.at[t, z], blocks.at[t, z], zu_sem, (t, z), up), has_up)
            send(copy_to(blocks.at[t, z], blocks.at[t, z], zd_sem, (t, z), down), has_down)
        if t == 0:
            send(ids_copy)
            one_hots(0, ids_ref)
        if t == 1:
            ids_copy.wait_recv()
            one_hots(1, ids_far)
        for k in range(1, lines):
            j = t - k
            if 0 <= j < chunks:
                low, high = z - k, z + k
                from_low = copy_to(blocks.at[j, low], blocks.at[j, low], zu_sem, (j, low), up)
                from_high = copy_to(blocks.at[j, high], blocks.at[j, high], zd_sem, (j, high), down)
                pl.when(low >= 0)(from_low.wait_recv)
                if k + 1 < lines:
                    send(from_low, (low >= 0) & has_up)
                pl.when(high < lines)(from_high.wait_recv)
                if k + 1 < lines:
                    send(from_high, (high < lines) & has_down)
        j = t - (lines - 1)
        if 0 <= j < chunks:
            found = blocks[j].reshape(lines * tok_rows, wide)
            far_send[j] = jnp.dot(pick[1], found, preferred_element_type=jnp.float32).astype(jnp.bfloat16)
            send(copy_to(far_send.at[j], far_recv.at[j], x_sem, (j,), x_peer))
            own_part[j] = jnp.dot(pick[0], found, preferred_element_type=jnp.float32)
        j = t - lines
        if 0 <= j < chunks:
            copy_to(far_send.at[j], far_recv.at[j], x_sem, (j,), x_peer).wait_recv()
            merged = (own_part[j] + far_recv[j].astype(jnp.float32)).astype(jnp.bfloat16)
            own_rows(j, dat)[...] = merged.reshape(experts_dev, cap_dev, wide)
            send(copy_to(own_rows(j, dat), own_rows(j, dat), y_sem, (j,), y_peer))
            send(copy_to(own_rows(j, dat), own_rows(j, dat), c_sem, (j,), c_peer))
            score = lax.dot_general(
                merged, router_ref[:, j * wide : (j + 1) * wide], (((1,), (1,)), ((), ())),
                preferred_element_type=jnp.float32,
            )
            row_id = lax.broadcasted_iota(jnp.int32, score.shape, 0)
            first = lax.broadcasted_iota(jnp.int32, score.shape, 1) * cap_dev
            mine = (row_id >= first) & (row_id < first + cap_dev)
            score = jnp.sum(jnp.where(mine, score, 0.0), axis=1, keepdims=True)
            gate[...] = score if j == 0 else gate[...] + score
        j = t - lines - 1
        if 0 <= j < chunks:
            copy_to(own_rows(j, dat_y), own_rows(j, dat_y), y_sem, (j,), y_peer).wait_recv()
            send(copy_to(own_rows(j, dat_y), own_rows(j, dat_y), cr_sem, (j,), c_peer))
        j = t - lines - 2
        if 0 <= j < chunks:
            copy_to(own_rows(j, dat_c), own_rows(j, dat_c), c_sem, (j,), c_peer).wait_recv()
            copy_to(own_rows(j, dat_yc), own_rows(j, dat_yc), cr_sem, (j,), c_peer).wait_recv()
            if (j + 1) % per == 0:
                first_product(j // per)
    gate[...] = jax.nn.sigmoid(gate[...])
    for e in range(experts_dev):
        loads[experts_dev + e].wait()

    def block(s):
        return slice(s * tok_rows, (s + 1) * tok_rows)

    for t in range(chunks + 4 + lines):
        j = t
        if j < chunks:
            if j % per == 0:

                @pl.loop(0, experts_dev, unroll=True)
                def _(e, j=j):
                    part = jnp.dot(
                        hidden[e], outer_v[e, :, j * wide : j * wide + span], preferred_element_type=jnp.float32
                    ).astype(jnp.bfloat16)
                    for d in range(PAIR * PAIR):
                        for k in range(per):
                            parts[j + k, d // PAIR, d % PAIR, e] = part[
                                d * cap_dev : (d + 1) * cap_dev, k * wide : (k + 1) * wide
                            ]

            send(copy_to(parts.at[j, :, 1 - c], core_recv.at[j], rc_sem, (j,), c_peer))
        j = t - 1
        if 0 <= j < chunks:
            copy_to(parts.at[j, :, 1 - c], core_recv.at[j], rc_sem, (j,), c_peer).wait_recv()
            theirs = parts[j, 1 - y, c].astype(jnp.float32) + core_recv[j, 1 - y].astype(jnp.float32)
            y_send[j] = theirs.astype(jnp.bfloat16).reshape(slots, wide)
            send(copy_to(y_send.at[j], y_recv.at[j], ry_sem, (j,), y_peer))
            ours = parts[j, y, c].astype(jnp.float32) + core_recv[j, y].astype(jnp.float32)
            kept[j] = ours.reshape(slots, wide)
        j = t - 2
        if 0 <= j < chunks:
            copy_to(y_send.at[j], y_recv.at[j], ry_sem, (j,), y_peer).wait_recv()
            summed = kept[j] + y_recv[j].astype(jnp.float32)
            weighted[j] = (gate[...] * summed).astype(jnp.bfloat16)
            send(copy_to(weighted.at[j], x_recv.at[j], rx_sem, (j,), x_peer))
        j = t - 3
        if 0 <= j < chunks:
            copy_to(weighted.at[j], x_recv.at[j], rx_sem, (j,), x_peer).wait_recv()
            spread = jnp.dot(place[0], weighted[j], preferred_element_type=jnp.float32)
            spread += jnp.dot(place[1], x_recv[j], preferred_element_type=jnp.float32)
            dense[j] = spread
        for s in range(lines):
            j = t - 3 - s
            if not 0 <= j < chunks:
                continue
            for dest in range(lines - 1, s, -1):
                here = z == s
                go = copy_to(up_send.at[j, dest], up_recv.at[j, dest], ru_sem, (j, dest), up)

                @pl.when(here)
                def _(j=j, dest=dest, s=s, go=go):
                    total = dense[j, block(dest), :]
                    if s > 0:
                        go.wait_recv()
                        total += up_recv[j, dest].astype(jnp.float32)
                    up_send[j, dest] = total.astype(jnp.bfloat16)

                send(go, here)
            top = lines - 1 - s
            for dest in range(top):
                here = z == top
                go = copy_to(down_send.at[j, dest], down_recv.at[j, dest], rd_sem, (j, dest), down)

                @pl.when(here)
                def _(j=j, dest=dest, top=top, go=go):
                    total = dense[j, block(dest), :]
                    if top < lines - 1:
                        go.wait_recv()
                        total += down_recv[j, dest].astype(jnp.float32)
                    down_send[j, dest] = total.astype(jnp.bfloat16)

                send(go, here)
        j = t - 3 - lines
        if 0 <= j < chunks:
            for s in range(lines):

                @pl.when(z == s)
                def _(j=j, s=s):
                    cols = slice(j * wide, (j + 1) * wide)
                    total = dense[j, block(s), :]
                    if s > 0:
                        copy_to(up_send.at[j, s], up_recv.at[j, s], ru_sem, (j, s), up).wait_recv()
                        total += up_recv[j, s].astype(jnp.float32)
                    if s < lines - 1:
                        copy_to(down_send.at[j, s], down_recv.at[j, s], rd_sem, (j, s), down).wait_recv()
                        total += down_recv[j, s].astype(jnp.float32)
                    out_ref[:, cols] = (tokens_ref[:, cols].astype(jnp.float32) + total).astype(jnp.bfloat16)

    for copy, cond in sent:
        if cond is None:
            copy.wait_send()
        else:
            pl.when(cond)(copy.wait_send)


def kernel_body(tokens, norm_gain, router_weight, inner_weight, outer_weight, slot_tokens, slot_ids):
    del slot_ids
    tok_rows, width = tokens.shape
    experts_dev, cap_dev = slot_tokens.shape
    units = inner_weight.shape[2]
    lines = lax.axis_size("exp") // PAIR
    dat_count = lax.axis_size("dat")
    slots = experts_dev * cap_dev
    chunks = width // CHUNK
    bf16, f32 = jnp.bfloat16, jnp.float32
    vmem = pl.BlockSpec(memory_space=pltpu.VMEM)
    hbm = pl.BlockSpec(memory_space=pl.ANY)
    dma = pltpu.SemaphoreType.DMA
    return pl.pallas_call(
        moe_kernel,
        out_shape=jax.ShapeDtypeStruct((tok_rows, width), bf16),
        in_specs=[vmem, vmem, vmem, vmem, hbm, hbm],
        out_specs=vmem,
        scratch_shapes=[
            pltpu.VMEM((experts_dev, width, units), bf16),
            pltpu.VMEM((experts_dev, units, width), bf16),
            pltpu.VMEM((experts_dev, cap_dev), jnp.int32),
            pltpu.VMEM((2, slots, lines * tok_rows), bf16),
            pltpu.VMEM((2, lines * tok_rows, slots), bf16),
            pltpu.VMEM((chunks, lines, tok_rows, CHUNK), bf16),
            pltpu.VMEM((chunks, slots, CHUNK), f32),
            pltpu.VMEM((chunks, slots, CHUNK), bf16),
            pltpu.VMEM((chunks, slots, CHUNK), bf16),
            pltpu.VMEM((width // GROUP, experts_dev, dat_count * cap_dev, GROUP), bf16),
            pltpu.VMEM((experts_dev, dat_count * cap_dev, units), f32),
            pltpu.VMEM((experts_dev, dat_count * cap_dev, units), bf16),
            pltpu.VMEM((slots, 1), f32),
            pltpu.VMEM((chunks, PAIR, PAIR, experts_dev, cap_dev, CHUNK), bf16),
            pltpu.VMEM((chunks, PAIR, experts_dev, cap_dev, CHUNK), bf16),
            pltpu.VMEM((chunks, slots, CHUNK), bf16),
            pltpu.VMEM((chunks, slots, CHUNK), bf16),
            pltpu.VMEM((chunks, slots, CHUNK), f32),
            pltpu.VMEM((chunks, slots, CHUNK), bf16),
            pltpu.VMEM((chunks, slots, CHUNK), bf16),
            pltpu.VMEM((chunks, lines * tok_rows, CHUNK), f32),
            pltpu.VMEM((chunks, lines, tok_rows, CHUNK), bf16),
            pltpu.VMEM((chunks, lines, tok_rows, CHUNK), bf16),
            pltpu.VMEM((chunks, lines, tok_rows, CHUNK), bf16),
            pltpu.VMEM((chunks, lines, tok_rows, CHUNK), bf16),
            dma((2, experts_dev)),
            dma((2,)),
            dma((2, chunks, lines)),
            dma((2, chunks, lines)),
            dma((2, chunks)),
            dma((2, chunks)),
            dma((2, chunks)),
            dma((2, chunks)),
            dma((2, chunks)),
            dma((2, chunks)),
            dma((2, chunks)),
            dma((2, chunks, lines)),
            dma((2, chunks, lines)),
        ],
        compiler_params=pltpu.CompilerParams(
            collective_id=0, has_side_effects=True, vmem_limit_bytes=60 * 1024 * 1024
        ),
    )(tokens, norm_gain.reshape(1, width), router_weight.T, slot_tokens, inner_weight, outer_weight)


def solution(mesh):
    chosen = kernel_body if mesh.shape["dat"] == PAIR * PAIR else body
    in_specs = (
        P(("exp", "dat"), None),
        P(),
        P(None, "exp"),
        P("exp", None, "dat"),
        P("exp", "dat", None),
        P("exp", "dat"),
        P(("exp", "dat"), None),
    )
    out_specs = P(("exp", "dat"), None)
    return jax.shard_map(chosen, mesh=mesh, in_specs=in_specs, out_specs=out_specs, check_vma=False)
```
